32 devices in a mesh: energy: 8 (over z, y), slab: 4 (over x, core).
Axes of the slice: x: 2, y: 2, z: 4, core: 2. Of those that a mesh axis runs over, the one named last changes fastest.
Arguments:
- green_blocks: bfloat16 [16, 4, 512, 512], P('energy', 'slab'), may hold values from -6 to 6
- coupling: bfloat16 [4, 512, 512], P('slab'), may hold values from -0.25 to 0.25
- coulomb: bfloat16 [4, 512, 512], P('slab'), may hold values from -0.25 to 0.25
Outputs:
- self_energy: bfloat16 [16, 4, 512, 512], P('energy', 'slab')
- screening: bfloat16 [16, 4, 512, 512], P('energy', 'slab')
The draws below stay inside these ranges and needn't reach their ends.
All inputs are finite; a program needn't handle non-finite values.
Results may differ from the reference program's by a relative error of at most 0.0075.
Values may be sent and summed in bfloat16 or wider, within the bound.
A program may use at most 64 MiB of HBM per device.

```python
import math
import jax
import jax.numpy as jnp
from jax import lax

M = 512
NE = 16
SLABS = 4


def levels(own_key, extent, cuts, smallest, largest):
    factor_of, own = 1.0, jax.random.fold_in(own_key, 6)
    for axis_at, shards_of in cuts:
        steps = jnp.exp(jax.random.uniform(jax.random.fold_in(own, axis_at), (shards_of,), jnp.float32, smallest / len(cuts), largest / len(cuts)))
        factor_of = factor_of * jnp.repeat(steps, extent[axis_at] // shards_of).reshape([-1 if axis == axis_at else 1 for axis in range(len(extent))])
    return factor_of


def noise(key, shape, width, bound, shards=(), kind=jnp.bfloat16):
    loudness = levels(key, shape, shards, -0.22, 0.18) if shards else 1.0
    array = jax.random.normal(key, shape, jnp.float32) * width * loudness
    return jnp.minimum(jnp.maximum(array, -bound), bound).astype(kind)


def setup_inputs(seed: int = 0) -> dict:
    key_of = jax.random.split(jax.random.key(seed), 4)
    return {
        "green_blocks": noise(key_of[0], (NE, SLABS, M, M), 1.0, 6.0, ((0, 8), (1, 4))),
        "coupling": noise(key_of[1], (SLABS, M, M), M ** -0.5, 0.25, ((0, 4),)),
        "coulomb": noise(key_of[2], (SLABS, M, M), M ** -0.5, 0.25, ((0, 4),)),
    }


def tables(count):
    indices = jnp.arange(count, dtype=jnp.int32)
    product = indices[:, None] * indices[None, :] % count
    angles = product.astype(jnp.float32) * (2.0 * math.pi / count)
    return (jnp.cos(angles), jnp.sin(angles))

def correlate(blocks):
    count = blocks.shape[0]
    cosine, sine = tables(count)
    flattened = blocks.astype(jnp.float32).reshape(count, -1)
    cosine_part = jnp.dot(cosine, flattened, precision=lax.Precision.HIGHEST)
    sine_part = jnp.dot(sine, flattened, precision=lax.Precision.HIGHEST)
    spectrum = cosine_part * cosine_part + sine_part * sine_part
    folded = jnp.dot(cosine, spectrum, precision=lax.Precision.HIGHEST) * (1.0 / (count * math.sqrt(count)))
    return folded.reshape(blocks.shape).astype(jnp.bfloat16)

def dress_lower(blocks, link):
    inner = jnp.einsum('eij,jk->eik', blocks.astype(jnp.float32), link.astype(jnp.float32)).astype(jnp.bfloat16)
    return jnp.einsum('ji,ejk->eik', link.astype(jnp.float32), inner.astype(jnp.float32)).astype(jnp.bfloat16)

def dress_upper(blocks, link):
    inner = jnp.einsum('eij,kj->eik', blocks.astype(jnp.float32), link.astype(jnp.float32)).astype(jnp.bfloat16)
    return jnp.einsum('ij,ejk->eik', link.astype(jnp.float32), inner.astype(jnp.float32)).astype(jnp.bfloat16)

def reference(green_blocks, coupling, coulomb):
    slab_ids = jnp.arange(SLABS, dtype=jnp.int32)

    def polar_slab(slab):
        return correlate(lax.dynamic_index_in_dim(green_blocks, slab, 1, False))
    polar = lax.map(polar_slab, slab_ids)

    def per_slab(slab):
        below = jnp.maximum(slab - 1, 0).astype(jnp.int32)
        above = jnp.minimum(slab + 1, SLABS - 1).astype(jnp.int32)
        has_below = (slab > 0).astype(jnp.float32)
        has_above = (slab < SLABS - 1).astype(jnp.float32)
        green_below = lax.dynamic_index_in_dim(green_blocks, below, 1, False)
        green_above = lax.dynamic_index_in_dim(green_blocks, above, 1, False)
        link_below = lax.dynamic_index_in_dim(coupling, below, 0, False)
        link_own = lax.dynamic_index_in_dim(coupling, slab, 0, False)
        lower = dress_lower(green_below, link_below).astype(jnp.float32) * has_below
        upper = dress_upper(green_above, link_own).astype(jnp.float32) * has_above
        sigma = (lower + upper).astype(jnp.bfloat16)
        polar_own = lax.dynamic_index_in_dim(polar, slab, 0, False)
        polar_below = lax.dynamic_index_in_dim(polar, below, 0, False).astype(jnp.float32) * has_below
        polar_above = lax.dynamic_index_in_dim(polar, above, 0, False).astype(jnp.float32) * has_above
        screen_block = lax.dynamic_index_in_dim(coulomb, slab, 0, False).astype(jnp.float32)
        inner = jnp.einsum('eij,kj->eik', polar_own.astype(jnp.float32), screen_block).astype(jnp.bfloat16)
        outer = jnp.einsum('ij,ejk->eik', screen_block, inner.astype(jnp.float32))
        screened = (outer + 0.5 * (polar_below + polar_above)).astype(jnp.bfloat16)
        return (sigma, screened)
    sigmas, screens = lax.map(per_slab, slab_ids)
    return (jnp.swapaxes(sigmas, 0, 1), jnp.swapaxes(screens, 0, 1))
```

```python
import functools

import jax
import jax.numpy as jnp
from jax import lax
from jax.experimental import pallas as pl
from jax.experimental.pallas import tpu as pltpu
from jax.sharding import PartitionSpec as P

MESH = pl.DeviceIdType.MESH
F32, BF16 = jnp.float32, jnp.bfloat16
TILE = 16
LANES = 128


def matmul(a, b, a_dim=1, b_dim=0):
    return lax.dot_general(a, b, (((a_dim,), (b_dim,)), ((), ())), preferred_element_type=F32)


def correlate(gath, prow, row0, rows):
    count, _, m = gath.shape
    scale = float(count) ** -0.5
    across = m // LANES

    def tile(i, _):
        r = pl.ds(pl.multiple_of(row0 + (i // across) * TILE, TILE), TILE)
        l = pl.ds(pl.multiple_of((i % across) * LANES, LANES), LANES)

        def put(w, total):
            value = (total * scale).astype(BF16)
            prow[w, r, l] = value
            return value

        if count <= 16:
            x = [gath[e, r, l].astype(F32) for e in range(count)]
            for w in range(count // 2 + 1):
                if 2 * w == count:
                    terms = [x[e] * x[e + w] for e in range(w)]
                else:
                    terms = [x[e] * x[(e + w) % count] for e in range(count)]
                while len(terms) > 1:
                    terms = [sum(terms[j : j + 2]) for j in range(0, len(terms), 2)]
                total = terms[0] * 2.0 if 2 * w == count else terms[0]
                value = put(w, total)
                if 0 < w < count - w:
                    prow[count - w, r, l] = value
        else:

            def lag(w, _):
                def term(e, total):
                    return total + gath[e, r, l].astype(F32) * gath[(e + w) % count, r, l].astype(F32)

                put(w, lax.fori_loop(0, count, term, jnp.zeros((TILE, LANES), F32)))
                return 0

            lax.fori_loop(0, count, lag, 0)
        return 0

    lax.fori_loop(0, (rows // TILE) * across, tile, 0)


def kernel(
    n, ns, parts, green, coupling, coulomb, sigma_out, screen_out,
    g, h, c, gath, prow, pol, inner, rim_b, rim_a, g_above, low_in, low_out, sigma, screen,
    local, ss1, rs1, ss2, rs2, ssb, rsb, ssa, rsa, sside, rside,
):
    per, m = g.shape[0], g.shape[1]
    rows = m // n // parts
    me, slab = lax.axis_index("energy"), lax.axis_index("slab")
    up, down = jnp.minimum(slab + 1, ns - 1), jnp.maximum(slab - 1, 0)
    has_up, has_down = slab < ns - 1, slab > 0
    order = sorted(range(1, n), key=lambda i: abs(2 * i - n))

    def block(part, owner):
        return pl.ds(pl.multiple_of(part * (m // parts) + owner * rows, rows), rows)

    loads = [
        pltpu.make_async_copy(green.at[:, 0], g, local.at[0]),
        pltpu.make_async_copy(coupling.at[0], h, local.at[1]),
        pltpu.make_async_copy(coulomb.at[0], c, local.at[2]),
    ]
    own = [
        pltpu.make_async_copy(
            green.at[:, 0, block(part, me)],
            gath.at[pl.ds(me * per, per), pl.ds(part * rows, rows)],
            local.at[3 + part],
        )
        for part in range(parts)
    ]
    for copy in loads + own:
        copy.start()

    barrier = pltpu.get_barrier_semaphore()
    for i in range(1, n):
        pl.semaphore_signal(barrier, inc=1, device_id={"energy": (me + i) % n}, device_id_type=MESH)

    @pl.when(has_up)
    def _():
        pl.semaphore_signal(barrier, inc=1, device_id={"slab": up}, device_id_type=MESH)

    @pl.when(has_down)
    def _():
        pl.semaphore_signal(barrier, inc=1, device_id={"slab": down}, device_id_type=MESH)

    pl.semaphore_wait(barrier, n - 1 + has_up.astype(jnp.int32) + has_down.astype(jnp.int32))

    def remote(src, dst, send, recv, where):
        return pltpu.make_async_remote_copy(
            src_ref=src, dst_ref=dst, send_sem=send, recv_sem=recv, device_id=where, device_id_type=MESH
        )

    loads[0].wait()
    first = {}
    for part in range(parts):
        for i in order:
            to = (me + i) % n
            first[part, i] = remote(
                g.at[:, block(part, to)],
                gath.at[pl.ds(me * per, per), pl.ds(part * rows, rows)],
                ss1.at[part, i], rs1.at[part, i], {"energy": to},
            )
            first[part, i].start()

    green_down = remote(g, g_above, sside.at[0], rside.at[0], {"slab": down})
    lower_up = remote(low_out, low_in, sside.at[1], rside.at[1], {"slab": up})

    @pl.when(has_down)
    def _():
        green_down.start()

    @pl.when(jnp.logical_not(has_down))
    def _():
        low_in[...] = jnp.zeros_like(low_in)
        rim_b[...] = jnp.zeros_like(rim_b)

    loads[1].wait()

    def lower(e, _):
        mid = matmul(g[e], h[...]).astype(BF16)
        low_out[e] = matmul(h[...], mid, 0, 0).astype(BF16)
        return 0

    lax.fori_loop(0, per, lower, 0)

    @pl.when(jnp.logical_not(has_up))
    def _():
        g_above[...] = jnp.zeros_like(g_above)
        rim_a[...] = jnp.zeros_like(rim_a)

    @pl.when(has_up)
    def _():
        lower_up.start()

    def self_energy():
        @pl.when(has_up)
        def _():
            green_down.wait_recv()

        @pl.when(has_down)
        def _():
            lower_up.wait_recv()

        def upper(e, _):
            mid = matmul(g_above[e], h[...], 1, 1).astype(BF16)
            term = matmul(h[...], mid).astype(BF16)
            sigma[e] = (low_in[e].astype(F32) + term.astype(F32)).astype(BF16)
            return 0

        lax.fori_loop(0, per, upper, 0)

    second, rims = {}, {}

    def forward(part, i):
        piece = block(part, (me - i + n) % n)
        rims[part, i] = (
            remote(pol.at[:, piece], rim_b.at[:, piece], ssb.at[part, i], rsb.at[part, i], {"slab": up}),
            remote(pol.at[:, piece], rim_a.at[:, piece], ssa.at[part, i], rsa.at[part, i], {"slab": down}),
        )

        @pl.when(has_up)
        def _():
            rims[part, i][0].start()

        @pl.when(has_down)
        def _():
            rims[part, i][1].start()

    for part in range(parts):
        own[part].wait()
        for i in order:
            first[part, i].wait_recv()
        correlate(gath, prow, part * rows, rows)
        span = pl.ds(part * rows, rows)
        pol[:, block(part, me)] = prow[pl.ds(me * per, per), span]
        for i in order:
            to = (me + i) % n
            second[part, i] = remote(
                prow.at[pl.ds(to * per, per), span], pol.at[:, block(part, me)],
                ss2.at[part, i], rs2.at[part, i], {"energy": to},
            )
            second[part, i].start()
        forward(part, 0)
    self_energy()
    sigma_store = pltpu.make_async_copy(sigma, sigma_out.at[:, 0], local.at[0])
    sigma_store.start()

    loads[2].wait()
    for part in range(parts):
        for i in order:
            second[part, i].wait_recv()
            forward(part, i)
        half = pl.ds(part * (m // parts), m // parts)

        def screen_inner(e, _):
            inner[e, half] = matmul(pol[e, half], c[...], 1, 1).astype(BF16)
            return 0

        lax.fori_loop(0, per, screen_inner, 0)

    for copies in rims.values():
        @pl.when(has_down)
        def _():
            copies[0].wait_recv()

        @pl.when(has_up)
        def _():
            copies[1].wait_recv()

    stores = []
    for e in range(per):
        beside = rim_b[e].astype(F32) + rim_a[e].astype(F32)
        screen[e] = (matmul(c[...], inner[e]) + 0.5 * beside).astype(BF16)
        stores.append(pltpu.make_async_copy(screen.at[e], screen_out.at[e, 0], local.at[1 + e]))
        stores[-1].start()

    for copy in list(first.values()) + list(second.values()):
        copy.wait_send()

    @pl.when(has_up)
    def _():
        lower_up.wait_send()
        for copies in rims.values():
            copies[0].wait_send()

    @pl.when(has_down)
    def _():
        green_down.wait_send()
        for copies in rims.values():
            copies[1].wait_send()

    sigma_store.wait()
    for copy in stores:
        copy.wait()


def solution(mesh):
    n, ns = mesh.shape["energy"], mesh.shape["slab"]

    def step(green, coupling, coulomb):
        per, m, count = green.shape[0], green.shape[-1], green.shape[0] * n
        parts = 2 if m // n % (2 * TILE) == 0 else 1
        rows = m // n
        blocks = pltpu.VMEM((per, m, m), BF16)
        square = pltpu.VMEM((m, m), BF16)
        strip = pltpu.VMEM((count, rows, m), BF16)
        sems = pltpu.SemaphoreType.DMA((parts, n))
        anywhere = pl.BlockSpec(memory_space=pl.ANY)
        return tuple(pl.pallas_call(
            functools.partial(kernel, n, ns, parts),
            out_shape=[jax.ShapeDtypeStruct(green.shape, BF16)] * 2,
            in_specs=[anywhere] * 3,
            out_specs=[anywhere] * 2,
            scratch_shapes=[blocks, square, square, strip, strip]
            + [blocks] * 9
            + [pltpu.SemaphoreType.DMA((max(3 + parts, 1 + per),))]
            + [sems] * 8
            + [pltpu.SemaphoreType.DMA((2,))] * 2,
            compiler_params=pltpu.CompilerParams(
                collective_id=0, has_side_effects=True, vmem_limit_bytes=67043328
            ),
        )(green, coupling, coulomb))

    placed = (P("energy", "slab", None, None), P("slab", None, None), P("slab", None, None))
    return jax.shard_map(
        step,
        mesh=mesh,
        in_specs=placed,
        out_specs=(P("energy", "slab", None, None),) * 2,
        check_vma=False,
    )
```

```python
import functools

import jax
import jax.numpy as jnp
from jax import lax
from jax.experimental import pallas as pl
from jax.experimental.pallas import tpu as pltpu
from jax.sharding import PartitionSpec as P

MESH = pl.DeviceIdType.MESH
F32, BF16 = jnp.float32, jnp.bfloat16
TILE = 16
LANES = 128


def matmul(a, b, a_dim=1, b_dim=0):
    return lax.dot_general(a, b, (((a_dim,), (b_dim,)), ((), ())), preferred_element_type=F32)


def correlate(gath, prow, row0, rows):
    count, _, m = gath.shape
    scale = float(count) ** -0.5
    across = m // LANES

    def tile(i, _):
        r = pl.ds(pl.multiple_of(row0 + (i // across) * TILE, TILE), TILE)
        l = pl.ds(pl.multiple_of((i % across) * LANES, LANES), LANES)

        def put(w, total):
            value = (total * scale).astype(BF16)
            prow[w, r, l] = value
            return value

        if count <= 16:
            x = [gath[e, r, l].astype(F32) for e in range(count)]
            for w in range(count // 2 + 1):
                if 2 * w == count:
                    terms = [x[e] * x[e + w] for e in range(w)]
                else:
                    terms = [x[e] * x[(e + w) % count] for e in range(count)]
                while len(terms) > 1:
                    terms = [sum(terms[j : j + 2]) for j in range(0, len(terms), 2)]
                total = terms[0] * 2.0 if 2 * w == count else terms[0]
                value = put(w, total)
                if 0 < w < count - w:
                    prow[count - w, r, l] = value
        else:

            def lag(w, _):
                def term(e, total):
                    return total + gath[e, r, l].astype(F32) * gath[(e + w) % count, r, l].astype(F32)

                put(w, lax.fori_loop(0, count, term, jnp.zeros((TILE, LANES), F32)))
                return 0

            lax.fori_loop(0, count, lag, 0)
        return 0

    lax.fori_loop(0, (rows // TILE) * across, tile, 0)


def kernel(
    n, ns, parts, green, coupling, coulomb, sigma, screen,
    g, h, c, gath, prow, pol, inner, rim_b, rim_a, g_above, low_in, low_out, outer,
    local, ss1, rs1, ss2, rs2, ssb, rsb, ssa, rsa, sside, rside,
):
    per, m = g.shape[0], g.shape[1]
    rows = m // n // parts
    me, slab = lax.axis_index("energy"), lax.axis_index("slab")
    up, down = jnp.minimum(slab + 1, ns - 1), jnp.maximum(slab - 1, 0)
    has_up, has_down = slab < ns - 1, slab > 0
    order = sorted(range(1, n), key=lambda i: abs(2 * i - n))

    def block(part, owner):
        return pl.ds(pl.multiple_of(part * (m // parts) + owner * rows, rows), rows)

    loads = [
        pltpu.make_async_copy(green.at[:, 0], g, local.at[0]),
        pltpu.make_async_copy(coupling.at[0], h, local.at[1]),
        pltpu.make_async_copy(coulomb.at[0], c, local.at[2]),
    ]
    own = [
        pltpu.make_async_copy(
            green.at[:, 0, block(part, me)],
            gath.at[pl.ds(me * per, per), pl.ds(part * rows, rows)],
            local.at[3 + part],
        )
        for part in range(parts)
    ]
    for copy in loads + own:
        copy.start()

    barrier = pltpu.get_barrier_semaphore()
    for i in range(1, n):
        pl.semaphore_signal(barrier, inc=1, device_id={"energy": (me + i) % n}, device_id_type=MESH)

    @pl.when(has_up)
    def _():
        pl.semaphore_signal(barrier, inc=1, device_id={"slab": up}, device_id_type=MESH)

    @pl.when(has_down)
    def _():
        pl.semaphore_signal(barrier, inc=1, device_id={"slab": down}, device_id_type=MESH)

    pl.semaphore_wait(barrier, n - 1 + has_up.astype(jnp.int32) + has_down.astype(jnp.int32))

    def remote(src, dst, send, recv, where):
        return pltpu.make_async_remote_copy(
            src_ref=src, dst_ref=dst, send_sem=send, recv_sem=recv, device_id=where, device_id_type=MESH
        )

    loads[0].wait()
    first = {}
    for part in range(parts):
        for i in order:
            to = (me + i) % n
            first[part, i] = remote(
                g.at[:, block(part, to)],
                gath.at[pl.ds(me * per, per), pl.ds(part * rows, rows)],
                ss1.at[part, i], rs1.at[part, i], {"energy": to},
            )
            first[part, i].start()

    green_down = remote(g, g_above, sside.at[0], rside.at[0], {"slab": down})
    lower_up = remote(low_out, low_in, sside.at[1], rside.at[1], {"slab": up})

    @pl.when(has_down)
    def _():
        green_down.start()

    @pl.when(jnp.logical_not(has_down))
    def _():
        low_in[...] = jnp.zeros_like(low_in)
        rim_b[...] = jnp.zeros_like(rim_b)

    loads[1].wait()

    def lower(e, _):
        mid = matmul(g[e], h[...]).astype(BF16)
        low_out[e] = matmul(h[...], mid, 0, 0).astype(BF16)
        return 0

    lax.fori_loop(0, per, lower, 0)

    @pl.when(jnp.logical_not(has_up))
    def _():
        g_above[...] = jnp.zeros_like(g_above)
        rim_a[...] = jnp.zeros_like(rim_a)

    @pl.when(has_up)
    def _():
        lower_up.start()

    def self_energy():
        @pl.when(has_up)
        def _():
            green_down.wait_recv()

        @pl.when(has_down)
        def _():
            lower_up.wait_recv()

        def upper(e, _):
            mid = matmul(g_above[e], h[...], 1, 1).astype(BF16)
            term = matmul(h[...], mid).astype(BF16)
            sigma[e, 0] = (low_in[e].astype(F32) + term.astype(F32)).astype(BF16)
            return 0

        lax.fori_loop(0, per, upper, 0)

    second, rims = {}, {}

    def forward(part, i):
        piece = block(part, (me - i + n) % n)
        rims[part, i] = (
            remote(pol.at[:, piece], rim_b.at[:, piece], ssb.at[part, i], rsb.at[part, i], {"slab": up}),
            remote(pol.at[:, piece], rim_a.at[:, piece], ssa.at[part, i], rsa.at[part, i], {"slab": down}),
        )

        @pl.when(has_up)
        def _():
            rims[part, i][0].start()

        @pl.when(has_down)
        def _():
            rims[part, i][1].start()

    for part in range(parts):
        own[part].wait()
        for i in order:
            first[part, i].wait_recv()
        correlate(gath, prow, part * rows, rows)
        span = pl.ds(part * rows, rows)
        pol[:, block(part, me)] = prow[pl.ds(me * per, per), span]
        for i in order:
            to = (me + i) % n
            second[part, i] = remote(
                prow.at[pl.ds(to * per, per), span], pol.at[:, block(part, me)],
                ss2.at[part, i], rs2.at[part, i], {"energy": to},
            )
            second[part, i].start()
        forward(part, 0)
    self_energy()

    loads[2].wait()
    for part in range(parts):
        for i in order:
            second[part, i].wait_recv()
            forward(part, i)
        half = pl.ds(part * (m // parts), m // parts)

        def screen_inner(e, _):
            inner[e, half] = matmul(pol[e, half], c[...], 1, 1).astype(BF16)
            return 0

        lax.fori_loop(0, per, screen_inner, 0)

    def screen_outer(e, _):
        outer[e] = matmul(c[...], inner[e])
        return 0

    lax.fori_loop(0, per, screen_outer, 0)

    for copies in rims.values():
        @pl.when(has_down)
        def _():
            copies[0].wait_recv()

        @pl.when(has_up)
        def _():
            copies[1].wait_recv()

    for e in range(per):
        beside = rim_b[e].astype(F32) + rim_a[e].astype(F32)
        screen[e, 0] = (outer[e] + 0.5 * beside).astype(BF16)

    for copy in list(first.values()) + list(second.values()):
        copy.wait_send()

    @pl.when(has_up)
    def _():
        lower_up.wait_send()
        for copies in rims.values():
            copies[0].wait_send()

    @pl.when(has_down)
    def _():
        green_down.wait_send()
        for copies in rims.values():
            copies[1].wait_send()


def store(sigma, screen, sigma_out, screen_out, sems):
    copies = [
        pltpu.make_async_copy(sigma, sigma_out, sems.at[0]),
        pltpu.make_async_copy(screen, screen_out, sems.at[1]),
    ]
    for copy in copies:
        copy.start()
    for copy in copies:
        copy.wait()


def solution(mesh):
    n, ns = mesh.shape["energy"], mesh.shape["slab"]

    def step(green, coupling, coulomb):
        per, m, count = green.shape[0], green.shape[-1], green.shape[0] * n
        parts = max(k for k in (1, 2) if m // n % (k * TILE) == 0)
        rows = m // n
        blocks = pltpu.VMEM((per, m, m), BF16)
        square = pltpu.VMEM((m, m), BF16)
        strip = pltpu.VMEM((count, rows, m), BF16)
        sems = pltpu.SemaphoreType.DMA((parts, n))
        shapes = [jax.ShapeDtypeStruct(green.shape, BF16)] * 2
        near = pl.BlockSpec(memory_space=pltpu.VMEM)
        far = pl.BlockSpec(memory_space=pltpu.HBM)
        held = pl.pallas_call(
            functools.partial(kernel, n, ns, parts),
            out_shape=shapes,
            in_specs=[far] * 3,
            out_specs=[near] * 2,
            scratch_shapes=[blocks, square, square, strip, strip]
            + [blocks] * 6
            + [blocks, pltpu.VMEM((per, m, m), F32)]
            + [pltpu.SemaphoreType.DMA((3 + parts,))]
            + [sems] * 8
            + [pltpu.SemaphoreType.DMA((2,))] * 2,
            compiler_params=pltpu.CompilerParams(
                collective_id=0, has_side_effects=True, vmem_limit_bytes=40 * 1024 * 1024
            ),
            name="step",
        )(*(pltpu.with_memory_space_constraint(x, pltpu.HBM) for x in (green, coupling, coulomb)))
        return tuple(
            pl.pallas_call(
                store,
                out_shape=shapes,
                in_specs=[near] * 2,
                out_specs=[far] * 2,
                scratch_shapes=[pltpu.SemaphoreType.DMA((2,))],
                compiler_params=pltpu.CompilerParams(vmem_limit_bytes=8 * 1024 * 1024),
                name="store",
            )(*held)
        )

    placed = (P("energy", "slab", None, None), P("slab", None, None), P("slab", None, None))
    return jax.shard_map(
        step,
        mesh=mesh,
        in_specs=placed,
        out_specs=(P("energy", "slab", None, None),) * 2,
        check_vma=False,
    )
```

```python
import functools

import jax
import jax.numpy as jnp
from jax import lax
from jax.experimental import pallas as pl
from jax.experimental.pallas import tpu as pltpu
from jax.sharding import PartitionSpec as P

MESH = pl.DeviceIdType.MESH
F32, BF16 = jnp.float32, jnp.bfloat16
TILE = 16
LANES = 128


def matmul(a, b, a_dim=1, b_dim=0):
    return lax.dot_general(a, b, (((a_dim,), (b_dim,)), ((), ())), preferred_element_type=F32)


def correlate(gath, prow, row0, rows):
    count, _, m = gath.shape
    scale = float(count) ** -0.5
    across = m // LANES

    def tile(i, _):
        r = pl.ds(pl.multiple_of(row0 + (i // across) * TILE, TILE), TILE)
        l = pl.ds(pl.multiple_of((i % across) * LANES, LANES), LANES)

        def put(w, total):
            value = (total * scale).astype(BF16)
            prow[w, r, l] = value
            return value

        if count <= 16:
            x = [gath[e, r, l].astype(F32) for e in range(count)]
            for w in range(count // 2 + 1):
                if 2 * w == count:
                    terms = [x[e] * x[e + w] for e in range(w)]
                else:
                    terms = [x[e] * x[(e + w) % count] for e in range(count)]
                while len(terms) > 1:
                    terms = [sum(terms[j : j + 2]) for j in range(0, len(terms), 2)]
                total = terms[0] * 2.0 if 2 * w == count else terms[0]
                value = put(w, total)
                if 0 < w < count - w:
                    prow[count - w, r, l] = value
        else:

            def lag(w, _):
                def term(e, total):
                    return total + gath[e, r, l].astype(F32) * gath[(e + w) % count, r, l].astype(F32)

                put(w, lax.fori_loop(0, count, term, jnp.zeros((TILE, LANES), F32)))
                return 0

            lax.fori_loop(0, count, lag, 0)
        return 0

    lax.fori_loop(0, (rows // TILE) * across, tile, 0)


def kernel(
    n, ns, parts, green, coupling, coulomb, sigma, screen,
    g, h, c, gath, prow, pol, inner, rim_b, rim_a, g_above, low_in, low_out, outer,
    local, ss1, rs1, ss2, rs2, ssb, rsb, ssa, rsa, sside, rside,
):
    per, m = g.shape[0], g.shape[1]
    rows = m // n // parts
    me, slab = lax.axis_index("energy"), lax.axis_index("slab")
    up, down = jnp.minimum(slab + 1, ns - 1), jnp.maximum(slab - 1, 0)
    has_up, has_down = slab < ns - 1, slab > 0
    order = range(1, n)

    def partner(i):
        other, bit = me, 1
        while bit <= i:
            if i & bit:
                other = other + bit * (1 - 2 * (me // bit % 2))
            bit *= 2
        return other


    def block(part, owner):
        return pl.ds(pl.multiple_of(part * (m // parts) + owner * rows, rows), rows)

    loads = [
        pltpu.make_async_copy(green.at[:, 0], g, local.at[0]),
        pltpu.make_async_copy(coupling.at[0], h, local.at[1]),
        pltpu.make_async_copy(coulomb.at[0], c, local.at[2]),
    ]
    own = [
        pltpu.make_async_copy(
            green.at[:, 0, block(part, me)],
            gath.at[pl.ds(me * per, per), pl.ds(part * rows, rows)],
            local.at[3 + part],
        )
        for part in range(parts)
    ]
    for copy in loads + own:
        copy.start()

    barrier = pltpu.get_barrier_semaphore()
    for i in range(1, n):
        pl.semaphore_signal(barrier, inc=1, device_id={"energy": (me + i) % n}, device_id_type=MESH)

    @pl.when(has_up)
    def _():
        pl.semaphore_signal(barrier, inc=1, device_id={"slab": up}, device_id_type=MESH)

    @pl.when(has_down)
    def _():
        pl.semaphore_signal(barrier, inc=1, device_id={"slab": down}, device_id_type=MESH)

    pl.semaphore_wait(barrier, n - 1 + has_up.astype(jnp.int32) + has_down.astype(jnp.int32))

    def remote(src, dst, send, recv, where):
        return pltpu.make_async_remote_copy(
            src_ref=src, dst_ref=dst, send_sem=send, recv_sem=recv, device_id=where, device_id_type=MESH
        )

    loads[0].wait()
    first = {}
    for part in range(parts):
        for i in order:
            to = partner(i)
            first[part, i] = remote(
                g.at[:, block(part, to)],
                gath.at[pl.ds(me * per, per), pl.ds(part * rows, rows)],
                ss1.at[part, i], rs1.at[part, i], {"energy": to},
            )
            first[part, i].start()

    green_down = remote(g, g_above, sside.at[0], rside.at[0], {"slab": down})
    lower_up = remote(low_out, low_in, sside.at[1], rside.at[1], {"slab": up})

    @pl.when(has_down)
    def _():
        green_down.start()

    @pl.when(jnp.logical_not(has_down))
    def _():
        low_in[...] = jnp.zeros_like(low_in)
        rim_b[...] = jnp.zeros_like(rim_b)

    loads[1].wait()

    def lower(e, _):
        mid = matmul(g[e], h[...]).astype(BF16)
        low_out[e] = matmul(h[...], mid, 0, 0).astype(BF16)
        return 0

    lax.fori_loop(0, per, lower, 0)

    @pl.when(jnp.logical_not(has_up))
    def _():
        g_above[...] = jnp.zeros_like(g_above)
        rim_a[...] = jnp.zeros_like(rim_a)

    @pl.when(has_up)
    def _():
        lower_up.start()

    def self_energy():
        @pl.when(has_up)
        def _():
            green_down.wait_recv()

        @pl.when(has_down)
        def _():
            lower_up.wait_recv()

        def upper(e, _):
            mid = matmul(g_above[e], h[...], 1, 1).astype(BF16)
            term = matmul(h[...], mid).astype(BF16)
            sigma[e, 0] = (low_in[e].astype(F32) + term.astype(F32)).astype(BF16)
            return 0

        lax.fori_loop(0, per, upper, 0)

    second, rims = {}, {}

    def forward(part, i):
        piece = block(part, partner(i))
        rims[part, i] = (
            remote(pol.at[:, piece], rim_b.at[:, piece], ssb.at[part, i], rsb.at[part, i], {"slab": up}),
            remote(pol.at[:, piece], rim_a.at[:, piece], ssa.at[part, i], rsa.at[part, i], {"slab": down}),
        )

        @pl.when(has_up)
        def _():
            rims[part, i][0].start()

        @pl.when(has_down)
        def _():
            rims[part, i][1].start()

    for part in range(parts):
        own[part].wait()
        for i in order:
            first[part, i].wait_recv()
        correlate(gath, prow, part * rows, rows)
        span = pl.ds(part * rows, rows)
        pol[:, block(part, me)] = prow[pl.ds(me * per, per), span]
        for i in order:
            to = partner(i)
            second[part, i] = remote(
                prow.at[pl.ds(to * per, per), span], pol.at[:, block(part, me)],
                ss2.at[part, i], rs2.at[part, i], {"energy": to},
            )
            second[part, i].start()
        forward(part, 0)
        if part == 0:
            self_energy()

    loads[2].wait()
    for part in range(parts):
        for i in order:
            second[part, i].wait_recv()
            forward(part, i)
        half = pl.ds(part * (m // parts), m // parts)

        def screen_inner(e, _):
            inner[e, half] = matmul(pol[e, half], c[...], 1, 1).astype(BF16)
            return 0

        lax.fori_loop(0, per, screen_inner, 0)

    def screen_outer(e, _):
        outer[e] = matmul(c[...], inner[e])
        return 0

    lax.fori_loop(0, per, screen_outer, 0)

    for part in range(parts):
        for i in range(n):
            @pl.when(has_down)
            def _():
                rims[part, i][0].wait_recv()

            @pl.when(has_up)
            def _():
                rims[part, i][1].wait_recv()

        half = pl.ds(part * (m // parts), m // parts)
        for e in range(per):
            beside = rim_b[e, half].astype(F32) + rim_a[e, half].astype(F32)
            screen[e, 0, half] = (outer[e, half] + 0.5 * beside).astype(BF16)

    for copy in list(first.values()) + list(second.values()):
        copy.wait_send()

    @pl.when(has_up)
    def _():
        lower_up.wait_send()
        for copies in rims.values():
            copies[0].wait_send()

    @pl.when(has_down)
    def _():
        green_down.wait_send()
        for copies in rims.values():
            copies[1].wait_send()


def store(sigma, screen, sigma_out, screen_out, sems):
    copies = [
        pltpu.make_async_copy(sigma, sigma_out, sems.at[0]),
        pltpu.make_async_copy(screen, screen_out, sems.at[1]),
    ]
    for copy in copies:
        copy.start()
    for copy in copies:
        copy.wait()


def solution(mesh):
    n, ns = mesh.shape["energy"], mesh.shape["slab"]
    assert n & (n - 1) == 0

    def step(green, coupling, coulomb):
        per, m, count = green.shape[0], green.shape[-1], green.shape[0] * n
        parts = max(k for k in (1, 2) if m // n % (k * TILE) == 0)
        rows = m // n
        blocks = pltpu.VMEM((per, m, m), BF16)
        square = pltpu.VMEM((m, m), BF16)
        strip = pltpu.VMEM((count, rows, m), BF16)
        sems = pltpu.SemaphoreType.DMA((parts, n))
        shapes = [jax.ShapeDtypeStruct(green.shape, BF16)] * 2
        near = pl.BlockSpec(memory_space=pltpu.VMEM)
        far = pl.BlockSpec(memory_space=pltpu.HBM)
        held = pl.pallas_call(
            functools.partial(kernel, n, ns, parts),
            out_shape=shapes,
            in_specs=[far] * 3,
            out_specs=[near] * 2,
            scratch_shapes=[blocks, square, square, strip, strip]
            + [blocks] * 6
            + [blocks, pltpu.VMEM((per, m, m), F32)]
            + [pltpu.SemaphoreType.DMA((3 + parts,))]
            + [sems] * 8
            + [pltpu.SemaphoreType.DMA((2,))] * 2,
            compiler_params=pltpu.CompilerParams(
                collective_id=0, has_side_effects=True, vmem_limit_bytes=40 * 1024 * 1024
            ),
            name="step",
        )(*(pltpu.with_memory_space_constraint(x, pltpu.HBM) for x in (green, coupling, coulomb)))
        return tuple(
            pl.pallas_call(
                store,
                out_shape=shapes,
                in_specs=[near] * 2,
                out_specs=[far] * 2,
                scratch_shapes=[pltpu.SemaphoreType.DMA((2,))],
                compiler_params=pltpu.CompilerParams(vmem_limit_bytes=8 * 1024 * 1024),
                name="store",
            )(*held)
        )

    placed = (P("energy", "slab", None, None), P("slab", None, None), P("slab", None, None))
    return jax.shard_map(
        step,
        mesh=mesh,
        in_specs=placed,
        out_specs=(P("energy", "slab", None, None),) * 2,
        check_vma=False,
    )
```
